512 devices in a mesh: group: 16 (over z), row: 8 (over x, core), col: 4 (over y).
Axes of the slice: x: 4, y: 4, z: 16, core: 2. Of those that a mesh axis runs over, the one named last changes fastest.
Arguments:
- child_front: float32 [16, 4, 4, 128, 2, 8, 128], P('group', None, 'col', None, None, 'row'), as said below
- top_front: float32 [12, 4, 16, 8, 6, 8, 128], P(None, 'col', 'group', None, None, 'row'), as said below
- block_map: int32 [16, 8], replicated, may hold values from 0 to 47, as said below
- pivots: int32 [16], P('group'), may hold values from 512 to 1024, as said below
- noise: float32 [16, 1024], P('group'), may hold values from -6 to 6
- top_sample: float32 [6144], replicated, may hold values from -12 to 12
Outputs:
- top_out: float32 [12, 4, 16, 8, 6, 8, 128], P(None, 'col', 'group', None, None, 'row')
- child_sample: float32 [16, 1024], P('group')
The draws below stay inside these ranges and needn't reach their ends.
Inputs may be any that keep to these rules, and one draw needn't show every extreme that they name: `child_front`: each child front is symmetric positive definite. `top_front`: symmetric positive definite. block_map[g, u] mod 8 equals u; the entries of one row are distinct. `pivots`: A multiple of 128; some child has 1024.
All inputs are finite; a program needn't handle non-finite values.
Results may differ from the reference program's by a relative error of at most 0.00015.
Values sent between devices are 32-bit elements; how exact they have to be, the bound alone decides.
No kernel may reach another device: no remote copies, remote signals or barrier semaphores. Data moves between devices by JAX's collectives and lax.ppermute only.
A program may use at most 64 MiB of HBM per device.

```python
import functools
import math
import jax
import jax.numpy as jnp
from jax import lax

BS = 128
CYCLE = 8
PC = 1024
UC = 1024
FP = 6144
FC = 2048
GROUPS = 16
N_GROUP = 16
N_ROW = 8
N_COL = 4


def positive_matrix(key, matrix_order):
    key_raw = jax.random.fold_in(key, 0)
    key_diagonal = jax.random.fold_in(key, 1)
    key_place = jax.random.fold_in(key, 3)
    raw = jax.random.normal(key_raw, (matrix_order, matrix_order), jnp.float32)
    coupling = (raw + raw.T) * (1.0 / math.sqrt(2.0 * matrix_order))
    diagonal = jax.random.uniform(key_diagonal, (matrix_order,), jnp.float32, 3.0, 5.0)
    places = jax.random.uniform(key_place, (2, matrix_order), jnp.float32, 0.0, 1.0)
    across = places[0][:, None] - places[0][None, :]
    along = places[1][:, None] - places[1][None, :]
    distance = jnp.sqrt(across * across + along * along)
    reach = 0.3
    kernel = 0.5 * jnp.exp(-distance / reach)
    matrix = coupling + kernel + jnp.diag(diagonal)
    return matrix


def draw_child_front(key, part):
    keys = jax.random.split(jax.random.fold_in(key, 11), GROUPS)
    fronts = jax.vmap(functools.partial(positive_matrix, matrix_order=FC))(keys)
    return fronts.reshape(GROUPS, FC // (BS * N_COL), N_COL, BS, FC // (BS * N_ROW), N_ROW, BS).astype(jnp.float32)


def draw_top_front(key, part):
    matrix = positive_matrix(jax.random.fold_in(key, 12), FP)
    return matrix.reshape(FP // (BS * N_COL), N_COL, N_GROUP, BS // N_GROUP, FP // (BS * N_ROW), N_ROW, BS).astype(jnp.float32)


def draw_block_map(key, part):
    shifts = jax.random.randint(jax.random.fold_in(key, 13), (GROUPS, UC // BS), 0, FP // (CYCLE * BS))
    places = jnp.arange(UC // BS, dtype=jnp.int32) % CYCLE
    return (shifts * CYCLE + places[None, :]).astype(jnp.int32)


def draw_pivots(key, part):
    key_count, key_full = jax.random.split(jax.random.fold_in(key, 14))
    counts = jax.random.randint(key_count, (GROUPS,), PC // (2 * BS), PC // BS + 1) * BS
    fullest = jax.random.randint(key_full, (), 0, GROUPS)
    return jnp.where(jnp.arange(GROUPS) == fullest, PC, counts).astype(jnp.int32)


def block_scale(own_key, shape, shards, smallest, top_value):
    gain, own = 1.0, jax.random.fold_in(own_key, 6)
    for axis_at, parts in shards:
        steps = jnp.exp(jax.random.uniform(jax.random.fold_in(own, axis_at), (parts,), jnp.float32, smallest / len(shards), top_value / len(shards)))
        gain = gain * jnp.repeat(steps, shape[axis_at] // parts).reshape([-1 if axis == axis_at else 1 for axis in range(len(shape))])
    return gain


def bell_draw(key, shape, spread, bound, shards=(), kind=jnp.bfloat16):
    loudness = block_scale(key, shape, shards, -0.22, 0.18) if shards else 1.0
    result = jax.random.normal(key, shape, jnp.float32) * spread * loudness
    return jnp.minimum(jnp.maximum(result, -bound), bound).astype(kind)


def setup_inputs(seed: int = 0) -> dict:
    splits = jax.random.split(jax.random.key(seed), 7)
    return {
        "child_front": draw_child_front(jax.random.fold_in(splits[6], 71), 0),
        "top_front": draw_top_front(jax.random.fold_in(splits[6], 71), 0),
        "block_map": draw_block_map(jax.random.fold_in(splits[6], 71), 0),
        "pivots": draw_pivots(jax.random.fold_in(splits[6], 71), 0),
        "noise": bell_draw(splits[4], (GROUPS, PC), 1.0, 6.0, ((0, 16),), jnp.float32),
        "top_sample": bell_draw(splits[5], (FP,), 2.0, 12.0, (), jnp.float32),
    }


HIGH = lax.Precision.HIGHEST

def eliminate(matrix, pivot_count, panel_width):
    matrix_order = matrix.shape[0]
    position = jnp.arange(matrix_order, dtype=jnp.int32)
    for panel_index in range(pivot_count // panel_width):
        first_pivot = panel_index * panel_width
        factor = jnp.linalg.cholesky(matrix[first_pivot:first_pivot + panel_width, first_pivot:first_pivot + panel_width])
        columns = lax.linalg.triangular_solve(factor, matrix[first_pivot:first_pivot + panel_width, :], left_side=True, lower=True)
        columns = jnp.where(position[None, :] >= first_pivot, columns, jnp.zeros_like(columns))
        matrix = matrix - jnp.dot(columns.T, columns, precision=HIGH)
        matrix = matrix.at[first_pivot:first_pivot + panel_width, :].set(columns)
    return matrix

def reference(child_front, top_front, block_map, pivots, noise, top_sample):
    panel_width = BS * N_COL
    top_matrix = top_front.reshape(FP, FP)
    position = jnp.arange(FC, dtype=jnp.int32)
    unit_matrix = jnp.eye(FC, dtype=top_matrix.dtype)
    offsets = jnp.arange(BS, dtype=jnp.int32)
    samples = []
    for group_index in range(GROUPS):
        child_matrix = child_front[group_index].reshape(FC, FC)
        dead_rows = (position < PC) & (position >= pivots[group_index])
        keep_mask = jnp.logical_not(dead_rows)[:, None] & jnp.logical_not(dead_rows)[None, :]
        child_matrix = jnp.where(keep_mask, child_matrix, unit_matrix)
        child_matrix = eliminate(child_matrix, PC, panel_width)
        targets = (block_map[group_index].astype(jnp.int32)[:, None] * BS + offsets[None, :]).reshape(-1).astype(jnp.int32)
        top_matrix = top_matrix.at[targets[:, None], targets[None, :]].add(child_matrix[PC:, PC:])
        coupled = top_sample[targets]
        right_side = noise[group_index] - jnp.dot(child_matrix[:PC, PC:], coupled, precision=HIGH)
        solved = lax.linalg.triangular_solve(child_matrix[:PC, :PC], right_side[:, None], left_side=True, lower=False)[:, 0]
        samples.append(solved)
    return (top_matrix.reshape(top_front.shape), jnp.stack(samples))
```

```python
import functools

import jax
import jax.numpy as jnp
from jax import lax
from jax.experimental import pallas as pl
from jax.experimental.pallas import tpu as pltpu
from jax.sharding import PartitionSpec as P

HIGH = lax.Precision.HIGHEST
F32 = jnp.float32
BF16 = jnp.bfloat16
B = 128
G = 8
PAIRS = [(i, i ^ 1) for i in range(8)]
PARITY = [[0, 2, 4, 6], [1, 3, 5, 7]]


def halves(x):
    high = x.astype(BF16)
    return high, (x - high.astype(F32)).astype(BF16)


def dot3(left, right, dims):
    lh, ll = halves(left)
    rh, rl = halves(right)

    def part(p, q):
        return lax.dot_general(p, q, (dims, ((), ())), preferred_element_type=F32)

    return part(lh, rh) + (part(lh, rl) + part(ll, rh))


def factor_block(vs):
    n = len(vs)
    sub = lax.broadcasted_iota(jnp.int32, (G, B), 0)
    lane = lax.broadcasted_iota(jnp.int32, (G, B), 1)
    vs = list(vs)
    out = []
    for g in range(n):
        base = g * G
        ingroup = (lane >= base) & (lane < base + G)
        cols = {}
        for v in range(g, n):
            for c in range(G):
                cols[v, c] = jnp.broadcast_to(vs[v][:, base + c : base + c + 1], (G, B))
        vs[g] = jnp.where(ingroup, jnp.where(lane - base == sub, 1.0, 0.0), vs[g])
        for v in range(g + 1, n):
            vs[v] = jnp.where(ingroup, 0.0, vs[v])
        dvec = jnp.ones((G, B), F32)
        for j in range(G):
            d = jnp.broadcast_to(cols[g, j][j : j + 1, :], (G, B))
            r = 1.0 / d
            dvec = jnp.where(sub == j, d, dvec)
            us = [
                jnp.broadcast_to(cols[g, c][j : j + 1, :], (G, B)) for c in range(j + 1, G)
            ]
            row = jnp.broadcast_to(vs[g][j : j + 1, :], (G, B))
            for v in range(g, n):
                f = cols[v, j] * r
                if v == g:
                    f = jnp.where(sub > j, f, 0.0)
                for i, c in enumerate(range(j + 1, G)):
                    cols[v, c] = cols[v, c] - f * us[i]
                vs[v] = vs[v] - f * row
        out.append(jnp.where(lane - base <= sub, vs[g] * lax.rsqrt(dvec), 0.0))
    return out


def child_kernel(
    par_ref, o0, o1, o2, q0, q1, q2, e_ref, co_ref, cq_ref, m_ref, n_ref,
    s_ref, x_ref, a_ref, lin_ref,
):
    nb = 8
    n = 12 * B
    even = par_ref[0] == 0
    owns, others = (o0, o1, o2), (q0, q1, q2)

    def rows_of(x, c, lo, hi):
        mine, theirs = [], []
        for p in range(3):
            a, b = max(lo, 88 * p), min(hi, 88 * p + 88)
            if a < b:
                mine.append(owns[p][x, c, a - 88 * p : b - 88 * p, :])
                theirs.append(others[p][x, c, a - 88 * p : b - 88 * p, :])
        mine = jnp.concatenate(mine, 0) if len(mine) > 1 else mine[0]
        theirs = jnp.concatenate(theirs, 0) if len(theirs) > 1 else theirs[0]
        return jnp.where(even, mine, theirs), jnp.where(even, theirs, mine)

    for c in range(4):
        sums = None
        for x in range(4):
            for lc in range(2):
                r0 = (4 * lc + c) * B
                b0, b1 = rows_of(x, c, lc * B, lc * B + B)
                a_ref[r0 : r0 + B, 2 * x * B : 2 * x * B + B] = b0
                a_ref[r0 : r0 + B, 2 * x * B + B : 2 * x * B + 2 * B] = b1
            t0, t1 = rows_of(x, c, 256, 264)
            sums = t0 + t1 if sums is None else sums + t0 + t1
        for lc in range(2):
            r0 = (4 * lc + c) * B
            a_ref[r0 : r0 + B, 11 * B :] = jnp.broadcast_to(sums[lc : lc + 1, :], (B, B)).T
            a_ref[r0 : r0 + B, 8 * B : 9 * B] = e_ref[c, lc * B : lc * B + B, :]
    for x in range(4):
        for lc in range(2):
            mine = co_ref[x, lc * B : lc * B + B, :]
            theirs = cq_ref[x, lc * B : lc * B + B, :]
            cs = slice((9 + lc) * B, (10 + lc) * B)
            a_ref[2 * x * B : 2 * x * B + B, cs] = jnp.where(even, mine, theirs).T
            a_ref[2 * x * B + B : 2 * x * B + 2 * B, cs] = jnp.where(even, theirs, mine).T

    def body(k, carry):
        off = pl.multiple_of(k * B, B)
        rows = factor_block(
            [a_ref[pl.ds(off + G * i, G), pl.ds(off, B)] for i in range(B // G)]
        )
        for i in range(B // G):
            lin_ref[pl.ds(off + G * i, G), :] = rows[i]
        for kk in range(nb):

            @pl.when(k == kk)
            def _():
                s, m = (kk + 1) * B, nb * B
                lin = lin_ref[kk * B : s, :]
                w = dot3(lin, a_ref[kk * B : s, s:], ((1,), (0,)))
                a_ref[kk * B : s, s:] = w
                if s < m:
                    low = dot3(a_ref[s:m, kk * B : s], lin, ((1,), (1,)))
                    a_ref[s:m, s:] = a_ref[s:m, s:] - dot3(low, w, ((1,), (0,)))

        return carry

    lax.fori_loop(0, nb, body, 0)

    prod = dot3(a_ref[:, 9 * B : 11 * B], a_ref[:, 8 * B : 9 * B], ((0,), (0,)))
    for b in range(2):
        for p in range(16):
            lo = b * B + G * p
            s_ref[p, b, :, :] = m_ref[lo : lo + G, :] - prod[lo : lo + G, :]

    xs = [None] * nb
    for k in reversed(range(nb)):
        ks = slice(k * B, k * B + B)
        z = jnp.broadcast_to(n_ref[:, ks], (B, B)).T - a_ref[ks, 11 * B :]
        if k + 1 < nb:
            acc = None
            for j in range(k + 1, nb):
                term = a_ref[ks, j * B : j * B + B] * xs[j]
                acc = term if acc is None else acc + term
            z = z - jnp.sum(acc, axis=1, keepdims=True)
        xs[k] = jnp.sum(lin_ref[ks, :] * z, axis=0, keepdims=True)
        x_ref[:, ks] = xs[k]


def local(child_front, top_front, block_map, pivots, noise, top_sample):
    my_row = lax.axis_index("row")
    my_col = lax.axis_index("col")
    my_group = lax.axis_index("group")
    pivot_total = noise.shape[1]
    tile = child_front.reshape(4, B, 2, B)
    live = pivots[0]
    lane = jnp.arange(B, dtype=jnp.int32)
    col_index = ((jnp.arange(4, dtype=jnp.int32) * 4 + my_col) * B)[:, None] + lane[None, :]
    row_index = ((jnp.arange(2, dtype=jnp.int32) * 8 + my_row) * B)[:, None] + lane[None, :]
    dead_c = (col_index < pivot_total) & (col_index >= live)
    dead_r = (row_index < pivot_total) & (row_index >= live)
    dead = dead_c[:, :, None, None] | dead_r[None, None, :, :]
    unit = (col_index[:, :, None, None] == row_index[None, None, :, :]).astype(F32)
    tile = jnp.where(dead, unit, tile)
    my_map = lax.dynamic_index_in_dim(block_map, my_group, 0, keepdims=False)
    known = lax.dynamic_index_in_dim(
        top_sample.reshape(-1, B), lax.dynamic_index_in_dim(my_map, my_row, 0, keepdims=False), 0
    )
    cross = tile[0:2, :, 1, :]
    partial_sum = jnp.sum(cross * known[None], axis=-1)
    first = jnp.concatenate(
        [tile[0:2, :, 0, :].reshape(2 * B, B), partial_sum, jnp.zeros((6, B), F32)], axis=0
    )
    wide = lax.all_gather(first, "col")
    cross_all = lax.all_gather(cross.reshape(2 * B, B), "col")
    own, other = [], []
    for p in range(3):
        got = lax.all_gather(wide[:, 88 * p : 88 * p + 88], "row", axis_index_groups=PARITY)
        own.append(got)
        other.append(lax.ppermute(got, "row", PAIRS))
    cols_own = lax.all_gather(
        tile[2:4, :, 0, :].reshape(2 * B, B), "row", axis_index_groups=PARITY
    )
    cols_other = lax.ppermute(cols_own, "row", PAIRS)
    vmem = pl.BlockSpec(memory_space=pltpu.VMEM)
    shares, solved = pl.pallas_call(
        child_kernel,
        out_shape=[
            jax.ShapeDtypeStruct((16, 2, G, B), F32),
            jax.ShapeDtypeStruct((1, pivot_total), F32),
        ],
        in_specs=[pl.BlockSpec(memory_space=pltpu.SMEM)] + [vmem] * 11,
        out_specs=[vmem, vmem],
        scratch_shapes=[pltpu.VMEM((8 * B, 12 * B), F32), pltpu.VMEM((8 * B, B), F32)],
        compiler_params=pltpu.CompilerParams(vmem_limit_bytes=48 * 2**20),
        name="child_front",
    )(
        (my_row % 2).astype(jnp.int32).reshape(1),
        *own,
        *other,
        cross_all,
        cols_own,
        cols_other,
        tile[2:4, :, 1, :].reshape(2 * B, B),
        noise,
    )
    arrived = lax.all_to_all(shares, "group", split_axis=0, concat_axis=0, tiled=True)

    col_blocks = jnp.arange(2, dtype=jnp.int32) * 4 + my_col
    col_target = jnp.take(block_map, col_blocks, axis=1) // 4
    row_target = lax.dynamic_index_in_dim(block_map, my_row, 1, keepdims=False) // 8
    top_cols = top_front.shape[0]
    top_rows = top_front.shape[4]
    col_hot = (
        col_target[:, :, None] == jnp.arange(top_cols, dtype=jnp.int32)[None, None, :]
    ).astype(F32)
    row_hot = (
        row_target[:, None] == jnp.arange(top_rows, dtype=jnp.int32)[None, :]
    ).astype(F32)
    top_tile = top_front.reshape(top_cols, G, top_rows, B)
    placed = row_hot[:, None, None, :, None] * arrived[:, :, :, None, :]
    top_tile = top_tile + jnp.einsum("gak,gamli->kmli", col_hot, placed, precision=HIGH)
    return (top_tile.reshape(top_front.shape), solved)


def solution(mesh):
    return jax.shard_map(
        local,
        mesh=mesh,
        in_specs=(
            P("group", None, "col", None, None, "row", None),
            P(None, "col", "group", None, None, "row", None),
            P(),
            P("group"),
            P("group", None),
            P(),
        ),
        out_specs=(P(None, "col", "group", None, None, "row", None), P("group", None)),
        check_vma=False,
    )
```

```python
import functools

import jax
import jax.numpy as jnp
from jax import lax
from jax.experimental import pallas as pl
from jax.experimental.pallas import tpu as pltpu
from jax.sharding import PartitionSpec as P

HIGH = lax.Precision.HIGHEST
F32 = jnp.float32
BF16 = jnp.bfloat16
B = 128
G = 8
HEAD = B + 8
PAIRS = [(i, i ^ 1) for i in range(8)]
PARITY = [[0, 2, 4, 6], [1, 3, 5, 7]]


def halves(x):
    high = x.astype(BF16)
    return high, (x - high.astype(F32)).astype(BF16)


def dot3(left, right, dims):
    lh, ll = halves(left)
    rh, rl = halves(right)

    def part(p, q):
        return lax.dot_general(p, q, (dims, ((), ())), preferred_element_type=F32)

    return part(lh, rh) + (part(lh, rl) + part(ll, rh))


def factor_block(vs):
    n = len(vs)
    sub = lax.broadcasted_iota(jnp.int32, (G, B), 0)
    lane = lax.broadcasted_iota(jnp.int32, (G, B), 1)
    vs = list(vs)
    out = []
    for g in range(n):
        base = g * G
        ingroup = (lane >= base) & (lane < base + G)
        cols = {}
        for v in range(g, n):
            for c in range(G):
                cols[v, c] = jnp.broadcast_to(vs[v][:, base + c : base + c + 1], (G, B))
        vs[g] = jnp.where(ingroup, jnp.where(lane - base == sub, 1.0, 0.0), vs[g])
        for v in range(g + 1, n):
            vs[v] = jnp.where(ingroup, 0.0, vs[v])
        dvec = jnp.ones((G, B), F32)
        for j in range(G):
            d = jnp.broadcast_to(cols[g, j][j : j + 1, :], (G, B))
            r = 1.0 / d
            dvec = jnp.where(sub == j, d, dvec)
            us = [
                jnp.broadcast_to(cols[g, c][j : j + 1, :], (G, B)) for c in range(j + 1, G)
            ]
            row = jnp.broadcast_to(vs[g][j : j + 1, :], (G, B))
            for v in range(g, n):
                f = cols[v, j] * r
                if v == g:
                    f = jnp.where(sub > j, f, 0.0)
                for i, c in enumerate(range(j + 1, G)):
                    cols[v, c] = cols[v, c] - f * us[i]
                vs[v] = vs[v] - f * row
        out.append(jnp.where(lane - base <= sub, vs[g] * lax.rsqrt(dvec), 0.0))
    return out


def front_kernel(f_ref, map_ref, piv_ref, y_ref, first_ref, cols_ref):
    my_row = lax.axis_index("row")
    my_col = lax.axis_index("col")
    my_group = lax.axis_index("group")
    live = piv_ref[0]
    shape = (B, B)
    i_id = lax.broadcasted_iota(jnp.int32, shape, 0)
    t_id = lax.broadcasted_iota(jnp.int32, shape, 1)

    def block(lc, lr):
        x = f_ref[pl.ds(2 * B * lc + lr, B, stride=2), :]
        ci = (4 * lc + my_col) * B + i_id
        ri = (8 * lr + my_row) * B + t_id
        if lc < 2 and lr == 0:
            dead = (ci >= live) | (ri >= live)
            return jnp.where(dead, jnp.where(ci == ri, 1.0, 0.0), x)
        return jnp.where((ci if lc < 2 else ri) >= live, 0.0, x)

    x0, x1 = block(0, 0), block(1, 0)
    step = (my_col - my_row + 8) % 8
    near = step < 4
    sent = jnp.where(near, x0, x1)
    rest = jnp.where(near, x1, x0)
    on_diagonal = step % 4 == 0
    first_ref[0:B, :] = jnp.where(on_diagonal & (i_id <= t_id), rest, sent)
    first_ref[B : B + 8, :] = jnp.zeros((8, B), F32)
    first_ref[B : B + 1, :] = jnp.sum(
        jnp.where(i_id == t_id, sent, 0.0), axis=0, keepdims=True
    )
    known = y_ref[pl.ds(map_ref[my_group, my_row], 1), :]
    for lc in range(2):
        x = block(lc, 1)
        first_ref[HEAD + lc * B : HEAD + lc * B + B, :] = x
        part = jnp.sum(x * known, axis=1, keepdims=True)
        first_ref[B + 1 + lc : B + 2 + lc, :] = jnp.sum(
            jnp.where(i_id == t_id, part, 0.0), axis=0, keepdims=True
        )
        cols_ref[lc * B : lc * B + B, :] = block(2 + lc, 0)


def chain_kernel(own_ref, other_ref, a_ref, lin_ref, v_ref):
    nb = 8
    m = nb * B
    even = lax.axis_index("row") % 2 == 0
    i_id = lax.broadcasted_iota(jnp.int32, (B, B), 0)
    t_id = lax.broadcasted_iota(jnp.int32, (B, B), 1)
    lower = i_id > t_id

    def rows_of(s, c, lo, hi):
        mine = own_ref[s // 2, c, lo:hi, :]
        theirs = other_ref[s // 2, c, lo:hi, :]
        return jnp.where(even, mine, theirs) if s % 2 == 0 else jnp.where(even, theirs, mine)

    def put(i, j, x):
        a_ref[i * B : i * B + B, j * B : j * B + B] = x

    sums = [None] * nb
    skew = [None] * nb
    for s in range(nb):
        for c in range(4):
            tail = rows_of(s, c, B, B + 8)
            for lc in range(2):
                j = 4 * lc + c
                got = tail[1 + lc : 2 + lc, :]
                sums[j] = got if sums[j] is None else sums[j] + got
            x = rows_of(s, c, 0, B)
            j = c if (c - s) % 8 < 4 else c + 4
            if j == s:
                low = jnp.where(lower, x, 0.0)
                put(s, s, low + low.T + jnp.where(i_id == t_id, tail[0:1, :], 0.0))
                skew[s] = x
            else:
                put(j, s, x)
                put(s, j, x.T)
    for s in range(4):
        z = jnp.where(lower, skew[s + 4].T, skew[s])
        put(s + 4, s, z)
        put(s, s + 4, z.T)
    for j in range(nb):
        v_ref[j : j + 1, :] = sums[j]

    def body(k, carry):
        off = pl.multiple_of(k * B, B)
        rows = factor_block(
            [a_ref[pl.ds(off + G * i, G), pl.ds(off, B)] for i in range(B // G)]
        )
        for i in range(B // G):
            lin_ref[pl.ds(off + G * i, G), :] = rows[i]
        for kk in range(nb - 1):

            @pl.when(k == kk)
            def _():
                s = (kk + 1) * B
                lin = lin_ref[kk * B : s, :]
                w = dot3(lin, a_ref[kk * B : s, s:m], ((1,), (0,)))
                a_ref[kk * B : s, s:m] = w
                low = dot3(a_ref[s:m, kk * B : s], lin, ((1,), (1,)))
                a_ref[s:m, kk * B : s] = low
                a_ref[s:m, s:m] = a_ref[s:m, s:m] - dot3(low, w, ((1,), (0,)))

        return carry

    lax.fori_loop(0, nb, body, 0)


def schur_kernel(a_ref, lin_ref, v_ref, e_ref, c_ref, f_ref, s_ref, t_ref, w_ref):
    nb = 8
    for k in range(nb):
        ks = slice(k * B, k * B + B)
        lc, c = k // 4, k % 4
        e = jnp.concatenate(
            [
                e_ref[c, HEAD + lc * B : HEAD + lc * B + B, :],
                c_ref[k, 0:B, :].T,
                c_ref[k, B : 2 * B, :].T,
                jnp.broadcast_to(v_ref[k : k + 1, :], (B, B)).T,
            ],
            axis=1,
        )
        if k:
            e = e - dot3(a_ref[ks, 0 : k * B], w_ref[0 : k * B, :], ((1,), (0,)))
        w_ref[ks, :] = dot3(lin_ref[ks, :], e, ((1,), (0,)))
    t_ref[...] = w_ref[:, 3 * B :]
    prod = dot3(w_ref[:, B : 3 * B], w_ref[:, 0:B], ((0,), (0,)))
    for b in range(2):
        x = f_ref[pl.ds(2 * B * (2 + b) + 1, B, stride=2), :] - prod[b * B : b * B + B, :]
        for p in range(16):
            s_ref[p, b, :, :] = x[G * p : G * p + G, :]


def sample_kernel(a_ref, lin_ref, t_ref, n_ref, x_ref):
    nb = 8
    xs = [None] * nb
    for k in reversed(range(nb)):
        ks = slice(k * B, k * B + B)
        z = jnp.broadcast_to(n_ref[:, ks], (B, B)).T - t_ref[ks, :]
        if k + 1 < nb:
            acc = None
            for j in range(k + 1, nb):
                term = a_ref[ks, j * B : j * B + B] * xs[j]
                acc = term if acc is None else acc + term
            z = z - jnp.sum(acc, axis=1, keepdims=True)
        xs[k] = jnp.sum(lin_ref[ks, :] * z, axis=0, keepdims=True)
        x_ref[:, ks] = xs[k]


def kernel_call(body, name, outs, scratch, flops, args, smem=()):
    specs = [
        pl.BlockSpec(memory_space=pltpu.SMEM if i in smem else pltpu.VMEM)
        for i in range(len(args))
    ]
    return pl.pallas_call(
        body,
        out_shape=[jax.ShapeDtypeStruct(s, F32) for s in outs],
        in_specs=specs,
        out_specs=[pl.BlockSpec(memory_space=pltpu.VMEM)] * len(outs),
        scratch_shapes=[pltpu.VMEM(s, F32) for s in scratch],
        compiler_params=pltpu.CompilerParams(vmem_limit_bytes=20 * 2**20),
        cost_estimate=pl.CostEstimate(
            flops=flops, bytes_accessed=8 * 2**20, transcendentals=0
        ),
        name=name,
    )(*args)


def local(child_front, top_front, block_map, pivots, noise, top_sample):
    my_row = lax.axis_index("row")
    my_col = lax.axis_index("col")
    front = child_front.reshape(8 * B, B)
    first, cols = kernel_call(
        front_kernel,
        "front",
        [(HEAD + 2 * B, B), (2 * B, B)],
        [],
        10**8,
        (front, block_map, pivots, top_sample.reshape(-1, B)),
        (1, 2),
    )
    wide = lax.all_gather(first, "col")
    own = lax.all_to_all(
        jnp.broadcast_to(wide[:, :HEAD], (4, 4, HEAD, B)),
        "row",
        split_axis=0,
        concat_axis=0,
        axis_index_groups=PARITY,
        tiled=True,
    )
    other = lax.ppermute(own, "row", PAIRS)
    own, other, cols = lax.optimization_barrier((own, other, cols))
    cols_all = lax.all_to_all(
        jnp.broadcast_to(cols, (8, 2 * B, B)), "row", split_axis=0, concat_axis=0, tiled=True
    )
    factor, inverses, coupled = kernel_call(
        chain_kernel,
        "chain",
        [(8 * B, 8 * B), (8 * B, B), (8, B)],
        [],
        4 * 10**9,
        (own, other),
    )
    shares, reduced = kernel_call(
        schur_kernel,
        "schur",
        [(16, 2, G, B), (8 * B, B)],
        [(8 * B, 4 * B)],
        10**9,
        (factor, inverses, coupled, wide, cols_all, front),
    )
    arrived = lax.all_to_all(shares, "group", split_axis=0, concat_axis=0, tiled=True)
    (solved,) = kernel_call(
        sample_kernel,
        "sample",
        [(1, 8 * B)],
        [],
        10**9,
        (factor, inverses, reduced, noise),
    )

    col_blocks = jnp.arange(2, dtype=jnp.int32) * 4 + my_col
    col_target = jnp.take(block_map, col_blocks, axis=1) // 4
    row_target = lax.dynamic_index_in_dim(block_map, my_row, 1, keepdims=False) // 8
    top_cols = top_front.shape[0]
    top_rows = top_front.shape[4]
    col_hot = (
        col_target[:, :, None] == jnp.arange(top_cols, dtype=jnp.int32)[None, None, :]
    ).astype(F32)
    row_hot = (
        row_target[:, None] == jnp.arange(top_rows, dtype=jnp.int32)[None, :]
    ).astype(F32)
    top_tile = top_front.reshape(top_cols, G, top_rows, B)
    placed = row_hot[:, None, None, :, None] * arrived[:, :, :, None, :]
    top_tile = top_tile + jnp.einsum("gak,gamli->kmli", col_hot, placed, precision=HIGH)
    return (top_tile.reshape(top_front.shape), solved)


def solution(mesh):
    return jax.shard_map(
        local,
        mesh=mesh,
        in_specs=(
            P("group", None, "col", None, None, "row", None),
            P(None, "col", "group", None, None, "row", None),
            P(),
            P("group"),
            P("group", None),
            P(),
        ),
        out_specs=(P(None, "col", "group", None, None, "row", None), P("group", None)),
        check_vma=False,
    )
```

```python
import functools

import jax
import jax.numpy as jnp
from jax import lax
from jax.experimental import pallas as pl
from jax.experimental.pallas import tpu as pltpu
from jax.sharding import PartitionSpec as P

HIGH = lax.Precision.HIGHEST
F32 = jnp.float32
BF16 = jnp.bfloat16
B = 128
G = 8
HEAD = B + 8
PAIRS = [(i, i ^ 1) for i in range(8)]
PARITY = [[0, 2, 4, 6], [1, 3, 5, 7]]


def halves(x):
    high = x.astype(BF16)
    return high, (x - high.astype(F32)).astype(BF16)


def dot3(left, right, dims):
    lh, ll = halves(left)
    rh, rl = halves(right)
    (ld,), (rd,) = dims
    return lax.dot_general(
        jnp.concatenate([lh, ll, lh], axis=ld),
        jnp.concatenate([rh, rh, rl], axis=rd),
        (dims, ((), ())),
        preferred_element_type=F32,
    )


def spread(x, j):
    return jnp.broadcast_to(x[j : j + 1, :], (G, B))


def factor_block(vs):
    n = len(vs)
    sub = lax.broadcasted_iota(jnp.int32, (G, B), 0)
    lane = lax.broadcasted_iota(jnp.int32, (G, B), 1)
    vs = list(vs)
    out = []
    for g in range(n):
        base = g * G
        ingroup = (lane >= base) & (lane < base + G)
        cols = {}
        for v in range(g, n):
            for c in range(G):
                cols[v, c] = jnp.take_along_axis(
                    vs[v],
                    jnp.full((G, B), base + c, jnp.int32),
                    axis=1,
                    mode="promise_in_bounds",
                )
        vs[g] = jnp.where(ingroup, jnp.where(lane - base == sub, 1.0, 0.0), vs[g])
        for v in range(g + 1, n):
            vs[v] = jnp.where(ingroup, 0.0, vs[v])
        dvec = jnp.ones((G, B), F32)
        d = spread(cols[g, 0], 0)
        for j in range(G):
            r = 1.0 / d
            dvec = jnp.where(sub == j, d, dvec)
            us = [spread(cols[g, c], j) for c in range(j + 1, G)]
            row = spread(vs[g], j)
            if j + 1 < G:
                d = spread(cols[g, j + 1], j + 1) - spread(cols[g, j], j + 1) * us[0] * r
            for v in range(g, n):
                f = cols[v, j] * r
                if v == g:
                    f = jnp.where(sub > j, f, 0.0)
                for i, c in enumerate(range(j + 1, G)):
                    cols[v, c] = cols[v, c] - f * us[i]
                vs[v] = vs[v] - f * row
        out.append(jnp.where(lane - base <= sub, vs[g] * lax.rsqrt(dvec), 0.0))
    return out


def front_kernel(f_ref, map_ref, piv_ref, y_ref, first_ref, cols_ref):
    my_row = lax.axis_index("row")
    my_col = lax.axis_index("col")
    my_group = lax.axis_index("group")
    live = piv_ref[0]
    shape = (B, B)
    i_id = lax.broadcasted_iota(jnp.int32, shape, 0)
    t_id = lax.broadcasted_iota(jnp.int32, shape, 1)

    def block(lc, lr):
        x = f_ref[pl.ds(2 * B * lc + lr, B, stride=2), :]
        ci = (4 * lc + my_col) * B + i_id
        ri = (8 * lr + my_row) * B + t_id
        if lc < 2 and lr == 0:
            dead = (ci >= live) | (ri >= live)
            return jnp.where(dead, jnp.where(ci == ri, 1.0, 0.0), x)
        return jnp.where((ci if lc < 2 else ri) >= live, 0.0, x)

    x0, x1 = block(0, 0), block(1, 0)
    step = (my_col - my_row + 8) % 8
    near = step < 4
    sent = jnp.where(near, x0, x1)
    rest = jnp.where(near, x1, x0)
    on_diagonal = step % 4 == 0
    first_ref[0:B, :] = jnp.where(on_diagonal & (i_id <= t_id), rest, sent)
    first_ref[B : B + 8, :] = jnp.zeros((8, B), F32)
    first_ref[B : B + 1, :] = jnp.sum(
        jnp.where(i_id == t_id, sent, 0.0), axis=0, keepdims=True
    )
    known = y_ref[pl.ds(map_ref[my_group, my_row], 1), :]
    for lc in range(2):
        x = block(lc, 1)
        first_ref[HEAD + lc * B : HEAD + lc * B + B, :] = x
        part = jnp.sum(x * known, axis=1, keepdims=True)
        first_ref[B + 1 + lc : B + 2 + lc, :] = jnp.sum(
            jnp.where(i_id == t_id, part, 0.0), axis=0, keepdims=True
        )
        cols_ref[lc * B : lc * B + B, :] = block(2 + lc, 0)


def chain_kernel(own_ref, other_ref, fac_ref, lin_ref, v_ref, a_ref, sems):
    nb = 8
    m = nb * B
    even = lax.axis_index("row") % 2 == 0
    i_id = lax.broadcasted_iota(jnp.int32, (B, B), 0)
    t_id = lax.broadcasted_iota(jnp.int32, (B, B), 1)
    lower = i_id > t_id

    def rows_of(s, c, lo, hi):
        mine = own_ref[s // 2, c, lo:hi, :]
        theirs = other_ref[s // 2, c, lo:hi, :]
        return jnp.where(even, mine, theirs) if s % 2 == 0 else jnp.where(even, theirs, mine)

    def put(i, j, x):
        a_ref[i * B : i * B + B, j * B : j * B + B] = x

    sums = [None] * nb
    skew = [None] * nb
    for s in range(nb):
        for c in range(4):
            tail = rows_of(s, c, B, B + 8)
            for lc in range(2):
                j = 4 * lc + c
                got = tail[1 + lc : 2 + lc, :]
                sums[j] = got if sums[j] is None else sums[j] + got
            x = rows_of(s, c, 0, B)
            j = c if (c - s) % 8 < 4 else c + 4
            if j == s:
                low = jnp.where(lower, x, 0.0)
                put(s, s, low + low.T + jnp.where(i_id == t_id, tail[0:1, :], 0.0))
                skew[s] = x
            else:
                put(j, s, x)
                put(s, j, x.T)
    for s in range(4):
        z = jnp.where(lower, skew[s + 4].T, skew[s])
        put(s + 4, s, z)
        put(s, s + 4, z.T)
    for j in range(nb):
        v_ref[j : j + 1, :] = sums[j]

    def row_copy(off, k):
        rows = pl.ds(off, B)
        return pltpu.make_async_copy(a_ref.at[rows, :], fac_ref.at[rows, :], sems.at[k])

    def body(k, carry):
        off = pl.multiple_of(k * B, B)
        rows = factor_block(
            [a_ref[pl.ds(off + G * i, G), pl.ds(off, B)] for i in range(B // G)]
        )
        for i in range(B // G):
            lin_ref[pl.ds(off + G * i, G), :] = rows[i]
        for kk in range(nb - 1):

            @pl.when(k == kk)
            def _():
                s = (kk + 1) * B
                lin = lin_ref[kk * B : s, :]
                w = dot3(lin, a_ref[kk * B : s, s:m], ((1,), (0,)))
                a_ref[kk * B : s, s:m] = w
                low = dot3(a_ref[s:m, kk * B : s], lin, ((1,), (1,)))
                a_ref[s:m, kk * B : s] = low
                a_ref[s:m, s:m] = a_ref[s:m, s:m] - dot3(low, w, ((1,), (0,)))

        row_copy(off, k).start()
        return carry

    lax.fori_loop(0, nb, body, 0)
    for k in range(nb):
        row_copy(k * B, k).wait()


def schur_kernel(
    fac_ref, lin_ref, v_ref, e_ref, c_ref, f_ref, s_ref, t_ref, w_ref, a_ref, sems
):
    nb = 8
    copies = [None]
    for k in range(1, nb):
        part = (pl.ds(k * B, B), pl.ds(0, k * B))
        copies.append(pltpu.make_async_copy(fac_ref.at[part], a_ref.at[part], sems.at[k]))
        copies[k].start()
    for k in range(nb):
        ks = slice(k * B, k * B + B)
        lc, c = k // 4, k % 4
        e = jnp.concatenate(
            [
                e_ref[c, HEAD + lc * B : HEAD + lc * B + B, :],
                c_ref[k, 0:B, :].T,
                c_ref[k, B : 2 * B, :].T,
                jnp.broadcast_to(v_ref[k : k + 1, :], (B, B)).T,
            ],
            axis=1,
        )
        if k:
            copies[k].wait()
            e = e - dot3(a_ref[ks, 0 : k * B], w_ref[0 : k * B, :], ((1,), (0,)))
        w_ref[ks, :] = dot3(lin_ref[ks, :], e, ((1,), (0,)))
    t_ref[...] = w_ref[:, 3 * B :]
    prod = dot3(w_ref[:, B : 3 * B], w_ref[:, 0:B], ((0,), (0,)))
    for b in range(2):
        x = f_ref[pl.ds(2 * B * (2 + b) + 1, B, stride=2), :] - prod[b * B : b * B + B, :]
        for p in range(16):
            s_ref[p, b, :, :] = x[G * p : G * p + G, :]


def sample_kernel(fac_ref, lin_ref, t_ref, n_ref, x_ref, a_ref, sems):
    nb = 8
    copies = {}
    for k in reversed(range(nb - 1)):
        part = (pl.ds(k * B, B), pl.ds((k + 1) * B, (nb - 1 - k) * B))
        copies[k] = pltpu.make_async_copy(fac_ref.at[part], a_ref.at[part], sems.at[k])
        copies[k].start()
    xs = [None] * nb
    for k in reversed(range(nb)):
        ks = slice(k * B, k * B + B)
        z = jnp.broadcast_to(n_ref[:, ks], (B, B)).T - t_ref[ks, :]
        if k + 1 < nb:
            copies[k].wait()
            acc = None
            for j in range(k + 1, nb):
                term = a_ref[ks, j * B : j * B + B] * xs[j]
                acc = term if acc is None else acc + term
            z = z - jnp.sum(acc, axis=1, keepdims=True)
        xs[k] = jnp.sum(lin_ref[ks, :] * z, axis=0, keepdims=True)
        x_ref[:, ks] = xs[k]


def kernel_call(body, name, outs, scratch, flops, args, smem=(), away=(), away_out=(), copies=0):
    def spec(space):
        return pl.BlockSpec(memory_space=space)

    ins = [
        spec(pltpu.SMEM if i in smem else pltpu.HBM if i in away else pltpu.VMEM)
        for i in range(len(args))
    ]
    results = [spec(pltpu.HBM if i in away_out else pltpu.VMEM) for i in range(len(outs))]
    scratch = [pltpu.VMEM(s, F32) for s in scratch]
    if copies:
        scratch.append(pltpu.SemaphoreType.DMA((copies,)))
    return pl.pallas_call(
        body,
        out_shape=[jax.ShapeDtypeStruct(s, F32) for s in outs],
        in_specs=ins,
        out_specs=results,
        scratch_shapes=scratch,
        compiler_params=pltpu.CompilerParams(vmem_limit_bytes=(60 if copies else 20) * 2**20),
        cost_estimate=pl.CostEstimate(
            flops=flops, bytes_accessed=8 * 2**20, transcendentals=0
        ),
        name=name,
    )(*args)


def local(child_front, top_front, block_map, pivots, noise, top_sample):
    my_row = lax.axis_index("row")
    my_col = lax.axis_index("col")
    front = child_front.reshape(8 * B, B)
    first, cols = kernel_call(
        front_kernel,
        "front",
        [(HEAD + 2 * B, B), (2 * B, B)],
        [],
        10**8,
        (front, block_map, pivots, top_sample.reshape(-1, B)),
        (1, 2),
    )
    wide = lax.all_gather(first, "col")
    own = lax.all_to_all(
        jnp.broadcast_to(wide[:, :HEAD], (4, 4, HEAD, B)),
        "row",
        split_axis=0,
        concat_axis=0,
        axis_index_groups=PARITY,
        tiled=True,
    )
    other = lax.ppermute(own, "row", PAIRS)
    cols, _ = lax.optimization_barrier((cols, other[0, 0, 0:8, :]))
    cols_all = lax.all_to_all(
        jnp.broadcast_to(cols, (8, 2 * B, B)), "row", split_axis=0, concat_axis=0, tiled=True
    )
    factor, inverses, coupled = kernel_call(
        chain_kernel,
        "chain",
        [(8 * B, 8 * B), (8 * B, B), (8, B)],
        [(8 * B, 8 * B)],
        4 * 10**9,
        (own, other),
        away_out=(0,),
        copies=8,
    )
    shares, reduced = kernel_call(
        schur_kernel,
        "schur",
        [(16, 2, G, B), (8 * B, B)],
        [(8 * B, 4 * B), (8 * B, 8 * B)],
        10**9,
        (factor, inverses, coupled, wide, cols_all, front),
        away=(0,),
        copies=8,
    )
    arrived = lax.all_to_all(shares, "group", split_axis=0, concat_axis=0, tiled=True)
    (solved,) = kernel_call(
        sample_kernel,
        "sample",
        [(1, 8 * B)],
        [(8 * B, 8 * B)],
        10**9,
        (factor, inverses, reduced, noise),
        away=(0,),
        copies=8,
    )

    col_blocks = jnp.arange(2, dtype=jnp.int32) * 4 + my_col
    col_target = jnp.take(block_map, col_blocks, axis=1) // 4
    row_target = lax.dynamic_index_in_dim(block_map, my_row, 1, keepdims=False) // 8
    top_cols = top_front.shape[0]
    top_rows = top_front.shape[4]
    col_hot = (
        col_target[:, :, None] == jnp.arange(top_cols, dtype=jnp.int32)[None, None, :]
    ).astype(F32)
    row_hot = (
        row_target[:, None] == jnp.arange(top_rows, dtype=jnp.int32)[None, :]
    ).astype(F32)
    top_tile = top_front.reshape(top_cols, G, top_rows, B)
    placed = row_hot[:, None, None, :, None] * arrived[:, :, :, None, :]
    top_tile = top_tile + jnp.einsum("gak,gamli->kmli", col_hot, placed, precision=HIGH)
    return (top_tile.reshape(top_front.shape), solved)


def solution(mesh):
    return jax.shard_map(
        local,
        mesh=mesh,
        in_specs=(
            P("group", None, "col", None, None, "row", None),
            P(None, "col", "group", None, None, "row", None),
            P(),
            P("group"),
            P("group", None),
            P(),
        ),
        out_specs=(P(None, "col", "group", None, None, "row", None), P("group", None)),
        check_vma=False,
    )
```

```python
import functools

import jax
import jax.numpy as jnp
from jax import lax
from jax.experimental import pallas as pl
from jax.experimental.pallas import tpu as pltpu
from jax.sharding import PartitionSpec as P

HIGH = lax.Precision.HIGHEST
F32 = jnp.float32
BF16 = jnp.bfloat16
B = 128
G = 8
HEAD = B + 8
PAIRS = [(i, i ^ 1) for i in range(8)]
PARITY = [[0, 2, 4, 6], [1, 3, 5, 7]]


def halves(x):
    high = x.astype(BF16)
    return high, (x - high.astype(F32)).astype(BF16)


def dot3(left, right, dims):
    lh, ll = halves(left)
    rh, rl = halves(right)
    (ld,), (rd,) = dims
    return lax.dot_general(
        jnp.concatenate([lh, ll, lh], axis=ld),
        jnp.concatenate([rh, rh, rl], axis=rd),
        (dims, ((), ())),
        preferred_element_type=F32,
    )


def spread(x, j):
    return jnp.broadcast_to(x[j : j + 1, :], (G, B))


def factor_block(vs):
    n = len(vs)
    pair, panel = 2, 8
    width = pair * G
    sub = lax.broadcasted_iota(jnp.int32, (G, B), 0)
    lane = lax.broadcasted_iota(jnp.int32, (G, B), 1)
    vs = list(vs)
    dvec = [jnp.ones((G, B), F32)] * n
    rvec = [jnp.ones((G, B), F32)] * n
    for p0 in range(0, n, panel):
        p1 = p0 + panel
        for g in range(p0, p1, pair):
            base = g * G
            ingroup = (lane >= base) & (lane < base + width)
            cols = {}
            for v in range(g, p1):
                for c in range(width):
                    cols[v, c] = jnp.take_along_axis(
                        vs[v],
                        jnp.full((G, B), base + c, jnp.int32),
                        axis=1,
                        mode="promise_in_bounds",
                    )
            for v in range(g, p1):
                own = jnp.where(lane - v * G == sub, 1.0, 0.0) if v < g + pair else 0.0
                vs[v] = jnp.where(ingroup, own, vs[v])
            d = spread(cols[g, 0], 0)
            for j in range(width):
                gv, row_at = g + j // G, j % G
                r = 1.0 / d
                dvec[gv] = jnp.where(sub == row_at, d, dvec[gv])
                rvec[gv] = jnp.where(sub == row_at, r, rvec[gv])
                us = [spread(cols[gv, c], row_at) for c in range(j + 1, width)]
                row = spread(vs[gv], row_at)
                if j + 1 < width:
                    gn, next_at = g + (j + 1) // G, (j + 1) % G
                    d = (
                        spread(cols[gn, j + 1], next_at)
                        - spread(cols[gn, j], next_at) * us[0] * r
                    )
                for v in range(gv, p1):
                    f = cols[v, j] * r
                    if v == gv:
                        f = jnp.where(sub > row_at, f, 0.0)
                    for i, c in enumerate(range(j + 1, width)):
                        cols[v, c] = cols[v, c] - f * us[i]
                    vs[v] = vs[v] - f * row
        if p1 < n:
            inside = (lane >= p0 * G) & (lane < p1 * G)
            rows = jnp.concatenate(
                [jnp.where(inside & (lane - g * G > sub), 0.0, vs[g]) for g in range(p0, p1)], 0
            )
            scaled = jnp.concatenate([vs[g] * rvec[g] for g in range(p0, p1)], 0)
            update = dot3(scaled, rows, ((0,), (0,)))
            for v in range(p1, n):
                vs[v] = jnp.where(inside, 0.0, vs[v]) - update[G * v : G * v + G, :]
    return [
        jnp.where(lane - g * G <= sub, vs[g] * lax.rsqrt(dvec[g]), 0.0) for g in range(n)
    ]


def front_kernel(f_ref, map_ref, piv_ref, y_ref, first_ref, cols_ref):
    my_row = lax.axis_index("row")
    my_col = lax.axis_index("col")
    my_group = lax.axis_index("group")
    live = piv_ref[0]
    shape = (B, B)
    i_id = lax.broadcasted_iota(jnp.int32, shape, 0)
    t_id = lax.broadcasted_iota(jnp.int32, shape, 1)

    def block(lc, lr):
        x = f_ref[pl.ds(2 * B * lc + lr, B, stride=2), :]
        ci = (4 * lc + my_col) * B + i_id
        ri = (8 * lr + my_row) * B + t_id
        if lc < 2 and lr == 0:
            dead = (ci >= live) | (ri >= live)
            return jnp.where(dead, jnp.where(ci == ri, 1.0, 0.0), x)
        return jnp.where((ci if lc < 2 else ri) >= live, 0.0, x)

    x0, x1 = block(0, 0), block(1, 0)
    step = (my_col - my_row + 8) % 8
    near = step < 4
    sent = jnp.where(near, x0, x1)
    rest = jnp.where(near, x1, x0)
    on_diagonal = step % 4 == 0
    first_ref[0:B, :] = jnp.where(on_diagonal & (i_id <= t_id), rest, sent)
    first_ref[B : B + 8, :] = jnp.zeros((8, B), F32)
    first_ref[B : B + 1, :] = jnp.sum(
        jnp.where(i_id == t_id, sent, 0.0), axis=0, keepdims=True
    )
    known = y_ref[pl.ds(map_ref[my_group, my_row], 1), :]
    for lc in range(2):
        x = block(lc, 1)
        first_ref[HEAD + lc * B : HEAD + lc * B + B, :] = x
        part = jnp.sum(x * known, axis=1, keepdims=True)
        first_ref[B + 1 + lc : B + 2 + lc, :] = jnp.sum(
            jnp.where(i_id == t_id, part, 0.0), axis=0, keepdims=True
        )
        cols_ref[lc * B : lc * B + B, :] = block(2 + lc, 0)


def chain_kernel(own_ref, other_ref, fac_ref, lin_ref, v_ref, a_ref, sems):
    nb = 8
    m = nb * B
    even = lax.axis_index("row") % 2 == 0
    i_id = lax.broadcasted_iota(jnp.int32, (B, B), 0)
    t_id = lax.broadcasted_iota(jnp.int32, (B, B), 1)
    lower = i_id > t_id

    def rows_of(s, c, lo, hi):
        mine = own_ref[s // 2, c, lo:hi, :]
        theirs = other_ref[s // 2, c, lo:hi, :]
        return jnp.where(even, mine, theirs) if s % 2 == 0 else jnp.where(even, theirs, mine)

    def put(i, j, x):
        a_ref[i * B : i * B + B, j * B : j * B + B] = x

    sums = [None] * nb
    skew = [None] * nb
    for s in range(nb):
        for c in range(4):
            tail = rows_of(s, c, B, B + 8)
            for lc in range(2):
                j = 4 * lc + c
                got = tail[1 + lc : 2 + lc, :]
                sums[j] = got if sums[j] is None else sums[j] + got
            x = rows_of(s, c, 0, B)
            j = c if (c - s) % 8 < 4 else c + 4
            if j == s:
                low = jnp.where(lower, x, 0.0)
                put(s, s, low + low.T + jnp.where(i_id == t_id, tail[0:1, :], 0.0))
                skew[s] = x
            else:
                put(j, s, x)
                put(s, j, x.T)
    for s in range(4):
        z = jnp.where(lower, skew[s + 4].T, skew[s])
        put(s + 4, s, z)
        put(s, s + 4, z.T)
    for j in range(nb):
        v_ref[j : j + 1, :] = sums[j]

    def row_copy(off, k):
        rows = pl.ds(off, B)
        return pltpu.make_async_copy(a_ref.at[rows, :], fac_ref.at[rows, :], sems.at[k])

    def body(k, carry):
        off = pl.multiple_of(k * B, B)
        rows = factor_block(
            [a_ref[pl.ds(off + G * i, G), pl.ds(off, B)] for i in range(B // G)]
        )
        for i in range(B // G):
            lin_ref[pl.ds(off + G * i, G), :] = rows[i]
        for kk in range(nb - 1):

            @pl.when(k == kk)
            def _():
                s = (kk + 1) * B
                lin = lin_ref[kk * B : s, :]
                w = dot3(lin, a_ref[kk * B : s, s:m], ((1,), (0,)))
                a_ref[kk * B : s, s:m] = w
                low = dot3(a_ref[s:m, kk * B : s], lin, ((1,), (1,)))
                a_ref[s:m, kk * B : s] = low
                a_ref[s:m, s:m] = a_ref[s:m, s:m] - dot3(low, w, ((1,), (0,)))

        row_copy(off, k).start()
        return carry

    lax.fori_loop(0, nb, body, 0)
    for k in range(nb):
        row_copy(k * B, k).wait()


def schur_kernel(
    fac_ref, lin_ref, v_ref, e_ref, c_ref, f_ref, s_ref, t_ref, a_ref, w_ref, sems
):
    nb = 8
    copies = [None]
    for k in range(1, nb):
        part = (pl.ds(k * B, B), pl.ds(0, k * B))
        copies.append(pltpu.make_async_copy(fac_ref.at[part], a_ref.at[part], sems.at[k]))
        copies[k].start()
    prod = None
    for k in range(nb):
        ks = slice(k * B, k * B + B)
        lc, c = k // 4, k % 4
        e = jnp.concatenate(
            [
                e_ref[c, HEAD + lc * B : HEAD + lc * B + B, :],
                c_ref[k, 0:B, :].T,
                c_ref[k, B : 2 * B, :].T,
                jnp.broadcast_to(v_ref[k : k + 1, :], (B, B)).T,
            ],
            axis=1,
        )
        if k:
            copies[k].wait()
            high, low = halves(a_ref[ks, 0 : k * B])
            left = []
            for j in range(k):
                js = slice(j * B, j * B + B)
                left += [high[:, js], low[:, js], high[:, js]]
            e = e - lax.dot_general(
                jnp.concatenate(left, axis=1),
                w_ref[0 : 3 * B * k, :],
                (((1,), (0,)), ((), ())),
                preferred_element_type=F32,
            )
        w = dot3(lin_ref[ks, :], e, ((1,), (0,)))
        t_ref[ks, :] = w[:, 3 * B :]
        if k + 1 < nb:
            high, low = halves(w)
            for i, x in enumerate((high, high, low)):
                w_ref[(3 * k + i) * B : (3 * k + i + 1) * B, :] = x
        term = dot3(w[:, B : 3 * B], w[:, 0:B], ((0,), (0,)))
        prod = term if prod is None else prod + term
    for b in range(2):
        x = f_ref[pl.ds(2 * B * (2 + b) + 1, B, stride=2), :] - prod[b * B : b * B + B, :]
        for p in range(16):
            s_ref[p, b, :, :] = x[G * p : G * p + G, :]


def sample_kernel(fac_ref, lin_ref, t_ref, n_ref, x_ref, a_ref, sems):
    nb = 8
    copies = {}
    for k in reversed(range(nb - 1)):
        part = (pl.ds(k * B, B), pl.ds((k + 1) * B, (nb - 1 - k) * B))
        copies[k] = pltpu.make_async_copy(fac_ref.at[part], a_ref.at[part], sems.at[k])
        copies[k].start()
    xs = [None] * nb
    for k in reversed(range(nb)):
        ks = slice(k * B, k * B + B)
        z = jnp.broadcast_to(n_ref[:, ks], (B, B)).T - t_ref[ks, :]
        if k + 1 < nb:
            copies[k].wait()
            acc = None
            for j in range(k + 1, nb):
                term = a_ref[ks, j * B : j * B + B] * xs[j]
                acc = term if acc is None else acc + term
            z = z - jnp.sum(acc, axis=1, keepdims=True)
        xs[k] = jnp.sum(lin_ref[ks, :] * z, axis=0, keepdims=True)
        x_ref[:, ks] = xs[k]


def kernel_call(body, name, outs, scratch, flops, args, smem=(), away=(), away_out=(), copies=0):
    def spec(space):
        return pl.BlockSpec(memory_space=space)

    ins = [
        spec(pltpu.SMEM if i in smem else pltpu.HBM if i in away else pltpu.VMEM)
        for i in range(len(args))
    ]
    results = [spec(pltpu.HBM if i in away_out else pltpu.VMEM) for i in range(len(outs))]
    scratch = [pltpu.VMEM(s, BF16 if s[0] > 8 * B else F32) for s in scratch]
    if copies:
        scratch.append(pltpu.SemaphoreType.DMA((copies,)))
    return pl.pallas_call(
        body,
        out_shape=[jax.ShapeDtypeStruct(s, F32) for s in outs],
        in_specs=ins,
        out_specs=results,
        scratch_shapes=scratch,
        compiler_params=pltpu.CompilerParams(vmem_limit_bytes=(50 if copies else 20) * 2**20),
        cost_estimate=pl.CostEstimate(
            flops=flops, bytes_accessed=8 * 2**20, transcendentals=0
        ),
        name=name,
    )(*args)


def local(child_front, top_front, block_map, pivots, noise, top_sample):
    my_row = lax.axis_index("row")
    my_col = lax.axis_index("col")
    front = child_front.reshape(8 * B, B)
    first, cols = kernel_call(
        front_kernel,
        "front",
        [(HEAD + 2 * B, B), (2 * B, B)],
        [],
        10**8,
        (front, block_map, pivots, top_sample.reshape(-1, B)),
        (1, 2),
    )
    wide = lax.all_gather(first, "col")
    own = lax.all_to_all(
        jnp.broadcast_to(wide[:, :HEAD], (4, 4, HEAD, B)),
        "row",
        split_axis=0,
        concat_axis=0,
        axis_index_groups=PARITY,
        tiled=True,
    )
    other = lax.ppermute(own, "row", PAIRS)
    cols, _ = lax.optimization_barrier((cols, other[0, 0, 0:8, :]))
    cols_all = lax.all_to_all(
        jnp.broadcast_to(cols, (8, 2 * B, B)), "row", split_axis=0, concat_axis=0, tiled=True
    )
    factor, inverses, coupled = kernel_call(
        chain_kernel,
        "chain",
        [(32 * B, 8 * B), (8 * B, B), (8, B)],
        [(8 * B, 8 * B)],
        4 * 10**9,
        (own, other),
        away_out=(0,),
        copies=8,
    )
    shares, reduced = kernel_call(
        schur_kernel,
        "schur",
        [(16, 2, G, B), (8 * B, B)],
        [(8 * B, 8 * B), (21 * B, 4 * B)],
        10**9,
        (factor, inverses, coupled, wide, cols_all, front),
        away=(0,),
        copies=8,
    )
    arrived = lax.all_to_all(shares, "group", split_axis=0, concat_axis=0, tiled=True)
    (solved,) = kernel_call(
        sample_kernel,
        "sample",
        [(1, 8 * B)],
        [(8 * B, 8 * B)],
        10**9,
        (factor, inverses, reduced, noise),
        away=(0,),
        copies=8,
    )

    col_blocks = jnp.arange(2, dtype=jnp.int32) * 4 + my_col
    col_target = jnp.take(block_map, col_blocks, axis=1) // 4
    row_target = lax.dynamic_index_in_dim(block_map, my_row, 1, keepdims=False) // 8
    top_cols = top_front.shape[0]
    top_rows = top_front.shape[4]
    col_hot = (
        col_target[:, :, None] == jnp.arange(top_cols, dtype=jnp.int32)[None, None, :]
    ).astype(F32)
    row_hot = (
        row_target[:, None] == jnp.arange(top_rows, dtype=jnp.int32)[None, :]
    ).astype(F32)
    top_tile = top_front.reshape(top_cols, G, top_rows, B)
    placed = row_hot[:, None, None, :, None] * arrived[:, :, :, None, :]
    top_tile = top_tile + jnp.einsum("gak,gamli->kmli", col_hot, placed, precision=HIGH)
    return (top_tile.reshape(top_front.shape), solved)


def solution(mesh):
    return jax.shard_map(
        local,
        mesh=mesh,
        in_specs=(
            P("group", None, "col", None, None, "row", None),
            P(None, "col", "group", None, None, "row", None),
            P(),
            P("group"),
            P("group", None),
            P(),
        ),
        out_specs=(P(None, "col", "group", None, None, "row", None), P("group", None)),
        check_vma=False,
    )
```

```python
import functools

import jax
import jax.numpy as jnp
from jax import lax
from jax.experimental import pallas as pl
from jax.experimental.pallas import tpu as pltpu
from jax.sharding import PartitionSpec as P

HIGH = lax.Precision.HIGHEST
F32 = jnp.float32
BF16 = jnp.bfloat16
B = 128
G = 8
HEAD = B + 8
PAIRS = [(i, i ^ 1) for i in range(8)]
PARITY = [[0, 2, 4, 6], [1, 3, 5, 7]]


def halves(x):
    high = x.astype(BF16)
    return high, (x - high.astype(F32)).astype(BF16)


def dot3(left, right, dims):
    lh, ll = halves(left)
    rh, rl = halves(right)
    (ld,), (rd,) = dims
    return lax.dot_general(
        jnp.concatenate([lh, ll, lh], axis=ld),
        jnp.concatenate([rh, rh, rl], axis=rd),
        (dims, ((), ())),
        preferred_element_type=F32,
    )


def spread(x, j):
    return jnp.broadcast_to(x[j : j + 1, :], (G, B))


def factor_block(vs):
    n = len(vs)
    pair, panel = 2, 8
    width = pair * G
    sub = lax.broadcasted_iota(jnp.int32, (G, B), 0)
    lane = lax.broadcasted_iota(jnp.int32, (G, B), 1)
    vs = list(vs)
    dvec = [jnp.ones((G, B), F32)] * n
    rvec = [jnp.ones((G, B), F32)] * n
    for p0 in range(0, n, panel):
        p1 = p0 + panel
        for g in range(p0, p1, pair):
            base = g * G
            ingroup = (lane >= base) & (lane < base + width)
            cols = {}
            for v in range(g, p1):
                for c in range(width):
                    cols[v, c] = jnp.take_along_axis(
                        vs[v],
                        jnp.full((G, B), base + c, jnp.int32),
                        axis=1,
                        mode="promise_in_bounds",
                    )
            for v in range(g, p1):
                own = jnp.where(lane - v * G == sub, 1.0, 0.0) if v < g + pair else 0.0
                vs[v] = jnp.where(ingroup, own, vs[v])
            d = spread(cols[g, 0], 0)
            for j in range(width):
                gv, row_at = g + j // G, j % G
                r = 1.0 / d
                dvec[gv] = jnp.where(sub == row_at, d, dvec[gv])
                rvec[gv] = jnp.where(sub == row_at, r, rvec[gv])
                us = [spread(cols[gv, c], row_at) for c in range(j + 1, width)]
                row = spread(vs[gv], row_at)
                if j + 1 < width:
                    gn, next_at = g + (j + 1) // G, (j + 1) % G
                    d = (
                        spread(cols[gn, j + 1], next_at)
                        - spread(cols[gn, j], next_at) * us[0] * r
                    )
                for v in range(gv, p1):
                    f = cols[v, j] * r
                    if v == gv:
                        f = jnp.where(sub > row_at, f, 0.0)
                    for i, c in enumerate(range(j + 1, width)):
                        cols[v, c] = cols[v, c] - f * us[i]
                    vs[v] = vs[v] - f * row
        if p1 < n:
            inside = (lane >= p0 * G) & (lane < p1 * G)
            rows = jnp.concatenate(
                [jnp.where(inside & (lane - g * G > sub), 0.0, vs[g]) for g in range(p0, p1)], 0
            )
            scaled = jnp.concatenate([vs[g] * rvec[g] for g in range(p0, p1)], 0)
            update = dot3(scaled, rows, ((0,), (0,)))
            for v in range(p1, n):
                vs[v] = jnp.where(inside, 0.0, vs[v]) - update[G * v : G * v + G, :]
    return [
        jnp.where(lane - g * G <= sub, vs[g] * lax.rsqrt(dvec[g]), 0.0) for g in range(n)
    ]


def front_kernel(f_ref, map_ref, piv_ref, y_ref, first_ref, cols_ref):
    my_row = lax.axis_index("row")
    my_col = lax.axis_index("col")
    my_group = lax.axis_index("group")
    live = piv_ref[0]
    shape = (B, B)
    i_id = lax.broadcasted_iota(jnp.int32, shape, 0)
    t_id = lax.broadcasted_iota(jnp.int32, shape, 1)

    def block(lc, lr):
        x = f_ref[pl.ds(2 * B * lc + lr, B, stride=2), :]
        ci = (4 * lc + my_col) * B + i_id
        ri = (8 * lr + my_row) * B + t_id
        if lc < 2 and lr == 0:
            dead = (ci >= live) | (ri >= live)
            return jnp.where(dead, jnp.where(ci == ri, 1.0, 0.0), x)
        return jnp.where((ci if lc < 2 else ri) >= live, 0.0, x)

    x0, x1 = block(0, 0), block(1, 0)
    step = (my_col - my_row + 8) % 8
    near = step < 4
    sent = jnp.where(near, x0, x1)
    rest = jnp.where(near, x1, x0)
    on_diagonal = step % 4 == 0
    first_ref[0:B, :] = jnp.where(on_diagonal & (i_id <= t_id), rest, sent)
    first_ref[B : B + 8, :] = jnp.zeros((8, B), F32)
    first_ref[B : B + 1, :] = jnp.sum(
        jnp.where(i_id == t_id, sent, 0.0), axis=0, keepdims=True
    )
    known = y_ref[pl.ds(map_ref[my_row, my_group], 1), :]
    for lc in range(2):
        x = block(lc, 1)
        first_ref[HEAD + lc * B : HEAD + lc * B + B, :] = x
        part = jnp.sum(x * known, axis=1, keepdims=True)
        first_ref[B + 1 + lc : B + 2 + lc, :] = jnp.sum(
            jnp.where(i_id == t_id, part, 0.0), axis=0, keepdims=True
        )
        cols_ref[lc * B : lc * B + B, :] = block(2 + lc, 0)


def chain_kernel(own_ref, other_ref, fac_ref, lin_ref, v_ref, a_ref, sems):
    nb = 8
    m = nb * B
    even = lax.axis_index("row") % 2 == 0
    i_id = lax.broadcasted_iota(jnp.int32, (B, B), 0)
    t_id = lax.broadcasted_iota(jnp.int32, (B, B), 1)
    lower = i_id > t_id

    def rows_of(s, c, lo, hi):
        mine = own_ref[s // 2, c, lo:hi, :]
        theirs = other_ref[s // 2, c, lo:hi, :]
        return jnp.where(even, mine, theirs) if s % 2 == 0 else jnp.where(even, theirs, mine)

    def put(i, j, x):
        a_ref[i * B : i * B + B, j * B : j * B + B] = x

    sums = [None] * nb
    skew = [None] * nb
    for s in range(nb):
        for c in range(4):
            tail = rows_of(s, c, B, B + 8)
            for lc in range(2):
                j = 4 * lc + c
                got = tail[1 + lc : 2 + lc, :]
                sums[j] = got if sums[j] is None else sums[j] + got
            x = rows_of(s, c, 0, B)
            j = c if (c - s) % 8 < 4 else c + 4
            if j == s:
                low = jnp.where(lower, x, 0.0)
                put(s, s, low + low.T + jnp.where(i_id == t_id, tail[0:1, :], 0.0))
                skew[s] = x
            else:
                put(j, s, x)
                put(s, j, x.T)
    for s in range(4):
        z = jnp.where(lower, skew[s + 4].T, skew[s])
        put(s + 4, s, z)
        put(s, s + 4, z.T)
    for j in range(nb):
        v_ref[j : j + 1, :] = sums[j]

    def row_copy(off, k):
        rows = pl.ds(off, B)
        return pltpu.make_async_copy(a_ref.at[rows, :], fac_ref.at[rows, :], sems.at[k])

    def body(k, carry):
        off = pl.multiple_of(k * B, B)
        rows = factor_block(
            [a_ref[pl.ds(off + G * i, G), pl.ds(off, B)] for i in range(B // G)]
        )
        for i in range(B // G):
            lin_ref[pl.ds(off + G * i, G), :] = rows[i]
        for kk in range(nb - 1):

            @pl.when(k == kk)
            def _():
                s = (kk + 1) * B
                lin = lin_ref[kk * B : s, :]
                w = dot3(lin, a_ref[kk * B : s, s:m], ((1,), (0,)))
                a_ref[kk * B : s, s:m] = w
                low = dot3(a_ref[s:m, kk * B : s], lin, ((1,), (1,)))
                a_ref[s:m, kk * B : s] = low
                a_ref[s:m, s:m] = a_ref[s:m, s:m] - dot3(low, w, ((1,), (0,)))

        row_copy(off, k).start()
        return carry

    lax.fori_loop(0, nb, body, 0)
    for k in range(nb):
        row_copy(k * B, k).wait()


def schur_kernel(
    fac_ref, lin_ref, v_ref, e_ref, c_ref, f_ref, s_ref, t_ref, a_ref, w_ref, sems
):
    nb = 8
    copies = [None]
    for k in range(1, nb):
        part = (pl.ds(k * B, B), pl.ds(0, k * B))
        copies.append(pltpu.make_async_copy(fac_ref.at[part], a_ref.at[part], sems.at[k]))
        copies[k].start()
    prod = None
    for k in range(nb):
        ks = slice(k * B, k * B + B)
        lc, c = k // 4, k % 4
        e = jnp.concatenate(
            [
                e_ref[c, HEAD + lc * B : HEAD + lc * B + B, :].T,
                c_ref[k, :, :],
                jnp.broadcast_to(v_ref[k : k + 1, :], (16, B)),
            ],
            axis=0,
        )
        if k:
            copies[k].wait()
            high, low = halves(a_ref[ks, 0 : k * B])
            right = []
            for j in range(k):
                js = slice(j * B, j * B + B)
                right += [high[:, js], low[:, js], high[:, js]]
            e = e - lax.dot_general(
                w_ref[:, 0 : 3 * B * k],
                jnp.concatenate(right, axis=1),
                (((1,), (1,)), ((), ())),
                preferred_element_type=F32,
            )
        w = dot3(e, lin_ref[ks, :], ((1,), (1,)))
        t_ref[k : k + 1, :] = w[3 * B : 3 * B + 1, :]
        if k + 1 < nb:
            high, low = halves(w)
            for i, x in enumerate((high, high, low)):
                w_ref[:, (3 * k + i) * B : (3 * k + i + 1) * B] = x
        term = dot3(w[B : 3 * B, :], w[0:B, :], ((1,), (1,)))
        prod = term if prod is None else prod + term
    for b in range(2):
        x = f_ref[pl.ds(2 * B * (2 + b) + 1, B, stride=2), :] - prod[b * B : b * B + B, :]
        for p in range(16):
            s_ref[p, b, :, :] = x[G * p : G * p + G, :]


def sample_kernel(fac_ref, lin_ref, t_ref, n_ref, x_ref, a_ref, sems):
    nb = 8
    copies = {}
    for k in reversed(range(nb - 1)):
        part = (pl.ds(k * B, B), pl.ds((k + 1) * B, (nb - 1 - k) * B))
        copies[k] = pltpu.make_async_copy(fac_ref.at[part], a_ref.at[part], sems.at[k])
        copies[k].start()
    xs = [None] * nb
    for k in reversed(range(nb)):
        ks = slice(k * B, k * B + B)
        z = jnp.broadcast_to(n_ref[:, ks] - t_ref[k : k + 1, :], (B, B)).T
        if k + 1 < nb:
            copies[k].wait()
            acc = None
            for j in range(k + 1, nb):
                term = a_ref[ks, j * B : j * B + B] * xs[j]
                acc = term if acc is None else acc + term
            z = z - jnp.sum(acc, axis=1, keepdims=True)
        xs[k] = jnp.sum(lin_ref[ks, :] * z, axis=0, keepdims=True)
        x_ref[:, ks] = xs[k]


def kernel_call(body, name, outs, scratch, flops, args, smem=(), away=(), away_out=(), copies=0):
    def spec(space):
        return pl.BlockSpec(memory_space=space)

    ins = [
        spec(pltpu.SMEM if i in smem else pltpu.HBM if i in away else pltpu.VMEM)
        for i in range(len(args))
    ]
    results = [spec(pltpu.HBM if i in away_out else pltpu.VMEM) for i in range(len(outs))]
    scratch = [pltpu.VMEM(s, BF16 if s[1] > 8 * B else F32) for s in scratch]
    if copies:
        scratch.append(pltpu.SemaphoreType.DMA((copies,)))
    return pl.pallas_call(
        body,
        out_shape=[jax.ShapeDtypeStruct(s, F32) for s in outs],
        in_specs=ins,
        out_specs=results,
        scratch_shapes=scratch,
        compiler_params=pltpu.CompilerParams(vmem_limit_bytes=(50 if copies else 20) * 2**20),
        cost_estimate=pl.CostEstimate(
            flops=flops, bytes_accessed=8 * 2**20, transcendentals=0
        ),
        name=name,
    )(*args)


def local(child_front, top_front, block_map, pivots, noise, top_sample):
    my_row = lax.axis_index("row")
    my_col = lax.axis_index("col")
    front = child_front.reshape(8 * B, B)
    first, cols = kernel_call(
        front_kernel,
        "front",
        [(HEAD + 2 * B, B), (2 * B, B)],
        [],
        10**8,
        (front, block_map.T, pivots, top_sample.reshape(-1, B)),
        (1, 2),
    )
    wide = lax.all_gather(first, "col")
    own = lax.all_to_all(
        jnp.broadcast_to(wide[:, :HEAD], (4, 4, HEAD, B)),
        "row",
        split_axis=0,
        concat_axis=0,
        axis_index_groups=PARITY,
        tiled=True,
    )
    other = lax.ppermute(own, "row", PAIRS)
    cols, _ = lax.optimization_barrier((cols, other[0, 0, 0:8, :]))
    cols_all = lax.all_to_all(
        jnp.broadcast_to(cols, (8, 2 * B, B)), "row", split_axis=0, concat_axis=0, tiled=True
    )
    factor, inverses, coupled = kernel_call(
        chain_kernel,
        "chain",
        [(32 * B, 8 * B), (8 * B, B), (8, B)],
        [(8 * B, 8 * B)],
        4 * 10**9,
        (own, other),
        away_out=(0,),
        copies=8,
    )
    shares, reduced = kernel_call(
        schur_kernel,
        "schur",
        [(16, 2, G, B), (8, B)],
        [(8 * B, 8 * B), (3 * B + 16, 21 * B)],
        10**9,
        (factor, inverses, coupled, wide, cols_all, front),
        away=(0,),
        copies=8,
    )
    arrived = lax.all_to_all(shares, "group", split_axis=0, concat_axis=0, tiled=True)
    (solved,) = kernel_call(
        sample_kernel,
        "sample",
        [(1, 8 * B)],
        [(8 * B, 8 * B)],
        10**9,
        (factor, inverses, reduced, noise),
        away=(0,),
        copies=8,
    )

    col_blocks = jnp.arange(2, dtype=jnp.int32) * 4 + my_col
    col_target = jnp.take(block_map, col_blocks, axis=1) // 4
    row_target = lax.dynamic_index_in_dim(block_map, my_row, 1, keepdims=False) // 8
    top_cols = top_front.shape[0]
    top_rows = top_front.shape[4]
    col_hot = (
        col_target[:, :, None] == jnp.arange(top_cols, dtype=jnp.int32)[None, None, :]
    ).astype(F32)
    row_hot = (
        row_target[:, None] == jnp.arange(top_rows, dtype=jnp.int32)[None, :]
    ).astype(F32)
    top_tile = top_front.reshape(top_cols, G, top_rows, B)
    placed = row_hot[:, None, None, :, None] * arrived[:, :, :, None, :]
    top_tile = top_tile + jnp.einsum("gak,gamli->kmli", col_hot, placed, precision=HIGH)
    return (top_tile.reshape(top_front.shape), solved)


def solution(mesh):
    return jax.shard_map(
        local,
        mesh=mesh,
        in_specs=(
            P("group", None, "col", None, None, "row", None),
            P(None, "col", "group", None, None, "row", None),
            P(),
            P("group"),
            P("group", None),
            P(),
        ),
        out_specs=(P(None, "col", "group", None, None, "row", None), P("group", None)),
        check_vma=False,
    )
```

```python
import functools

import jax
import jax.numpy as jnp
from jax import lax
from jax.experimental import pallas as pl
from jax.experimental.pallas import tpu as pltpu
from jax.sharding import PartitionSpec as P

HIGH = lax.Precision.HIGHEST
F32 = jnp.float32
BF16 = jnp.bfloat16
B = 128
G = 8
HEAD = B + 8
PAIRS = [(i, i ^ 1) for i in range(8)]
PARITY = [[0, 2, 4, 6], [1, 3, 5, 7]]


def halves(x):
    high = x.astype(BF16)
    return high, (x - high.astype(F32)).astype(BF16)


def dot3(left, right, dims):
    lh, ll = halves(left)
    rh, rl = halves(right)
    (ld,), (rd,) = dims
    return lax.dot_general(
        jnp.concatenate([lh, ll, lh], axis=ld),
        jnp.concatenate([rh, rh, rl], axis=rd),
        (dims, ((), ())),
        preferred_element_type=F32,
    )


def spread(x, j):
    return jnp.broadcast_to(x[j : j + 1, :], (G, B))


def factor_block(vs):
    n = len(vs)
    pair, panel = 2, 8
    width = pair * G
    sub = lax.broadcasted_iota(jnp.int32, (G, B), 0)
    lane = lax.broadcasted_iota(jnp.int32, (G, B), 1)
    vs = list(vs)
    dvec = [jnp.ones((G, B), F32)] * n
    rvec = [jnp.ones((G, B), F32)] * n
    for p0 in range(0, n, panel):
        p1 = p0 + panel
        for g in range(p0, p1, pair):
            base = g * G
            ingroup = (lane >= base) & (lane < base + width)
            cols = {}
            for v in range(g, p1):
                for c in range(width):
                    cols[v, c] = jnp.take_along_axis(
                        vs[v],
                        jnp.full((G, B), base + c, jnp.int32),
                        axis=1,
                        mode="promise_in_bounds",
                    )
            for v in range(g, p1):
                own = jnp.where(lane - v * G == sub, 1.0, 0.0) if v < g + pair else 0.0
                vs[v] = jnp.where(ingroup, own, vs[v])
            d = spread(cols[g, 0], 0)
            for j in range(width):
                gv, row_at = g + j // G, j % G
                r = 1.0 / d
                dvec[gv] = jnp.where(sub == row_at, d, dvec[gv])
                rvec[gv] = jnp.where(sub == row_at, r, rvec[gv])
                us = [spread(cols[gv, c], row_at) for c in range(j + 1, width)]
                row = spread(vs[gv], row_at)
                if j + 1 < width:
                    gn, next_at = g + (j + 1) // G, (j + 1) % G
                    d = (
                        spread(cols[gn, j + 1], next_at)
                        - spread(cols[gn, j], next_at) * us[0] * r
                    )
                for v in range(gv, p1):
                    f = cols[v, j] * r
                    if v == gv:
                        f = jnp.where(sub > row_at, f, 0.0)
                    for i, c in enumerate(range(j + 1, width)):
                        cols[v, c] = cols[v, c] - f * us[i]
                    vs[v] = vs[v] - f * row
        if p1 < n:
            inside = (lane >= p0 * G) & (lane < p1 * G)
            rows = jnp.concatenate(
                [jnp.where(inside & (lane - g * G > sub), 0.0, vs[g]) for g in range(p0, p1)], 0
            )
            scaled = jnp.concatenate([vs[g] * rvec[g] for g in range(p0, p1)], 0)
            update = dot3(scaled, rows, ((0,), (0,)))
            for v in range(p1, n):
                vs[v] = jnp.where(inside, 0.0, vs[v]) - update[G * v : G * v + G, :]
    return [
        jnp.where(lane - g * G <= sub, vs[g] * lax.rsqrt(dvec[g]), 0.0) for g in range(n)
    ]


def front_kernel(f_ref, map_ref, piv_ref, y_ref, first_ref, cols_ref):
    my_row = lax.axis_index("row")
    my_col = lax.axis_index("col")
    my_group = lax.axis_index("group")
    live = piv_ref[0]
    shape = (B, B)
    i_id = lax.broadcasted_iota(jnp.int32, shape, 0)
    t_id = lax.broadcasted_iota(jnp.int32, shape, 1)

    def block(lc, lr):
        x = f_ref[pl.ds(2 * B * lc + lr, B, stride=2), :]
        ci = (4 * lc + my_col) * B + i_id
        ri = (8 * lr + my_row) * B + t_id
        if lc < 2 and lr == 0:
            dead = (ci >= live) | (ri >= live)
            return jnp.where(dead, jnp.where(ci == ri, 1.0, 0.0), x)
        return jnp.where((ci if lc < 2 else ri) >= live, 0.0, x)

    x0, x1 = block(0, 0), block(1, 0)
    step = (my_col - my_row + 8) % 8
    near = step < 4
    sent = jnp.where(near, x0, x1)
    rest = jnp.where(near, x1, x0)
    on_diagonal = step % 4 == 0
    first_ref[0:B, :] = jnp.where(on_diagonal & (i_id <= t_id), rest, sent)
    first_ref[B : B + 8, :] = jnp.zeros((8, B), F32)
    first_ref[B : B + 1, :] = jnp.sum(
        jnp.where(i_id == t_id, sent, 0.0), axis=0, keepdims=True
    )
    known = y_ref[pl.ds(map_ref[my_group, my_row], 1), :]
    for lc in range(2):
        x = block(lc, 1)
        first_ref[HEAD + lc * B : HEAD + lc * B + B, :] = x
        part = jnp.sum(x * known, axis=1, keepdims=True)
        first_ref[B + 1 + lc : B + 2 + lc, :] = jnp.sum(
            jnp.where(i_id == t_id, part, 0.0), axis=0, keepdims=True
        )
        cols_ref[lc * B : lc * B + B, :] = block(2 + lc, 0)


def chain_kernel(own_ref, other_ref, fac_ref, lin_ref, v_ref, a_ref, sems):
    nb = 8
    m = nb * B
    even = lax.axis_index("row") % 2 == 0
    i_id = lax.broadcasted_iota(jnp.int32, (B, B), 0)
    t_id = lax.broadcasted_iota(jnp.int32, (B, B), 1)
    lower = i_id > t_id

    def rows_of(s, c, lo, hi):
        mine = own_ref[s // 2, c, lo:hi, :]
        theirs = other_ref[s // 2, c, lo:hi, :]
        return jnp.where(even, mine, theirs) if s % 2 == 0 else jnp.where(even, theirs, mine)

    def put(i, j, x):
        a_ref[i * B : i * B + B, j * B : j * B + B] = x

    sums = [None] * nb
    skew = [None] * nb
    for s in range(nb):
        for c in range(4):
            tail = rows_of(s, c, B, B + 8)
            for lc in range(2):
                j = 4 * lc + c
                got = tail[1 + lc : 2 + lc, :]
                sums[j] = got if sums[j] is None else sums[j] + got
            x = rows_of(s, c, 0, B)
            j = c if (c - s) % 8 < 4 else c + 4
            if j == s:
                low = jnp.where(lower, x, 0.0)
                put(s, s, low + low.T + jnp.where(i_id == t_id, tail[0:1, :], 0.0))
                skew[s] = x
            else:
                put(j, s, x)
                put(s, j, x.T)
    for s in range(4):
        z = jnp.where(lower, skew[s + 4].T, skew[s])
        put(s + 4, s, z)
        put(s, s + 4, z.T)
    for j in range(nb):
        v_ref[j : j + 1, :] = sums[j]

    def row_copy(off, k):
        rows = pl.ds(off, B)
        return pltpu.make_async_copy(a_ref.at[rows, :], fac_ref.at[rows, :], sems.at[k])

    def body(k, carry):
        off = pl.multiple_of(k * B, B)
        rows = factor_block(
            [a_ref[pl.ds(off + G * i, G), pl.ds(off, B)] for i in range(B // G)]
        )
        for i in range(B // G):
            lin_ref[pl.ds(off + G * i, G), :] = rows[i]
        for kk in range(nb - 1):

            @pl.when(k == kk)
            def _():
                s = (kk + 1) * B
                lin = lin_ref[kk * B : s, :]
                w = dot3(lin, a_ref[kk * B : s, s:m], ((1,), (0,)))
                a_ref[kk * B : s, s:m] = w
                low = dot3(a_ref[s:m, kk * B : s], lin, ((1,), (1,)))
                a_ref[s:m, kk * B : s] = low
                a_ref[s:m, s:m] = a_ref[s:m, s:m] - dot3(low, w, ((1,), (0,)))

        row_copy(off, k).start()
        return carry

    lax.fori_loop(0, nb, body, 0)
    for k in range(nb):
        row_copy(k * B, k).wait()


def schur_kernel(
    fac_ref, lin_ref, v_ref, e_ref, c_ref, f_ref, s_ref, t_ref, a_ref, w_ref, sems
):
    nb = 8
    copies = [None]
    for k in range(1, nb):
        part = (pl.ds(k * B, B), pl.ds(0, k * B))
        copies.append(pltpu.make_async_copy(fac_ref.at[part], a_ref.at[part], sems.at[k]))
        copies[k].start()
    prod = None
    for k in range(nb):
        ks = slice(k * B, k * B + B)
        lc, c = k // 4, k % 4
        e = jnp.concatenate(
            [
                e_ref[c, HEAD + lc * B : HEAD + lc * B + B, :],
                c_ref[k, 0:B, :].T,
                c_ref[k, B : 2 * B, :].T,
                jnp.broadcast_to(v_ref[k : k + 1, :], (B, B)).T,
            ],
            axis=1,
        )
        if k:
            copies[k].wait()
            high, low = halves(a_ref[ks, 0 : k * B])
            left = []
            for j in range(k):
                js = slice(j * B, j * B + B)
                left += [high[:, js], low[:, js], high[:, js]]
            e = e - lax.dot_general(
                jnp.concatenate(left, axis=1),
                w_ref[0 : 3 * B * k, :],
                (((1,), (0,)), ((), ())),
                preferred_element_type=F32,
            )
        w = dot3(lin_ref[ks, :], e, ((1,), (0,)))
        t_ref[ks, :] = w[:, 3 * B :]
        if k + 1 < nb:
            high, low = halves(w)
            for i, x in enumerate((high, high, low)):
                w_ref[(3 * k + i) * B : (3 * k + i + 1) * B, :] = x
        term = dot3(w[:, B : 3 * B], w[:, 0:B], ((0,), (0,)))
        prod = term if prod is None else prod + term
    for b in range(2):
        x = f_ref[pl.ds(2 * B * (2 + b) + 1, B, stride=2), :] - prod[b * B : b * B + B, :]
        for p in range(16):
            s_ref[p, b, :, :] = x[G * p : G * p + G, :]


def sample_kernel(fac_ref, lin_ref, t_ref, n_ref, x_ref, a_ref, sems):
    nb = 8
    copies = {}
    for k in reversed(range(nb - 1)):
        part = (pl.ds(k * B, B), pl.ds((k + 1) * B, (nb - 1 - k) * B))
        copies[k] = pltpu.make_async_copy(fac_ref.at[part], a_ref.at[part], sems.at[k])
        copies[k].start()
    xs = [None] * nb
    for k in reversed(range(nb)):
        ks = slice(k * B, k * B + B)
        z = jnp.broadcast_to(n_ref[:, ks], (B, B)).T - t_ref[ks, :]
        if k + 1 < nb:
            copies[k].wait()
            acc = None
            for j in range(k + 1, nb):
                term = a_ref[ks, j * B : j * B + B] * xs[j]
                acc = term if acc is None else acc + term
            z = z - jnp.sum(acc, axis=1, keepdims=True)
        xs[k] = jnp.sum(lin_ref[ks, :] * z, axis=0, keepdims=True)
        x_ref[:, ks] = xs[k]


def place_kernel(map_ref, top_ref, got_ref, out_ref):
    my_row = lax.axis_index("row")
    my_col = lax.axis_index("col")
    out_ref[...] = top_ref[...]
    for g in range(16):
        row = map_ref[g, my_row] >> 3
        for b in range(2):
            col = map_ref[g, 4 * b + my_col] >> 2
            rows = pl.ds(col * (6 * G) + row, G, stride=6)
            out_ref[rows, :] = out_ref[rows, :] + got_ref[g, b, :, :]


def kernel_call(body, name, outs, scratch, flops, args, smem=(), away=(), away_out=(), copies=0):
    def spec(space):
        return pl.BlockSpec(memory_space=space)

    ins = [
        spec(pltpu.SMEM if i in smem else pltpu.HBM if i in away else pltpu.VMEM)
        for i in range(len(args))
    ]
    results = [spec(pltpu.HBM if i in away_out else pltpu.VMEM) for i in range(len(outs))]
    scratch = [pltpu.VMEM(s, BF16 if s[0] > 8 * B else F32) for s in scratch]
    if copies:
        scratch.append(pltpu.SemaphoreType.DMA((copies,)))
    return pl.pallas_call(
        body,
        out_shape=[jax.ShapeDtypeStruct(s, F32) for s in outs],
        in_specs=ins,
        out_specs=results,
        scratch_shapes=scratch,
        compiler_params=pltpu.CompilerParams(vmem_limit_bytes=(50 if copies else 20) * 2**20),
        cost_estimate=pl.CostEstimate(
            flops=flops, bytes_accessed=8 * 2**20, transcendentals=0
        ),
        name=name,
    )(*args)


def local(child_front, top_front, block_map, pivots, noise, top_sample):
    front = child_front.reshape(8 * B, B)
    first, cols = kernel_call(
        front_kernel,
        "front",
        [(HEAD + 2 * B, B), (2 * B, B)],
        [],
        10**8,
        (front, block_map, pivots, top_sample.reshape(-1, B)),
        (1, 2),
    )
    wide = lax.all_gather(first, "col")
    own = lax.all_to_all(
        jnp.broadcast_to(wide[:, :HEAD], (4, 4, HEAD, B)),
        "row",
        split_axis=0,
        concat_axis=0,
        axis_index_groups=PARITY,
        tiled=True,
    )
    other = lax.ppermute(own, "row", PAIRS)
    cols, _ = lax.optimization_barrier((cols, other[0, 0, 0:8, :]))
    cols_all = lax.all_to_all(
        jnp.broadcast_to(cols, (8, 2 * B, B)), "row", split_axis=0, concat_axis=0, tiled=True
    )
    factor, inverses, coupled = kernel_call(
        chain_kernel,
        "chain",
        [(32 * B, 8 * B), (8 * B, B), (8, B)],
        [(8 * B, 8 * B)],
        4 * 10**9,
        (own, other),
        away_out=(0,),
        copies=8,
    )
    shares, reduced = kernel_call(
        schur_kernel,
        "schur",
        [(16, 2, G, B), (8 * B, B)],
        [(8 * B, 8 * B), (21 * B, 4 * B)],
        10**9,
        (factor, inverses, coupled, wide, cols_all, front),
        away=(0,),
        copies=8,
    )
    arrived = lax.all_to_all(shares, "group", split_axis=0, concat_axis=0, tiled=True)
    (solved,) = kernel_call(
        sample_kernel,
        "sample",
        [(1, 8 * B)],
        [(8 * B, 8 * B)],
        10**9,
        (factor, inverses, reduced, noise),
        away=(0,),
        copies=8,
    )

    (top_out,) = kernel_call(
        place_kernel,
        "place",
        [(12 * 6 * G, B)],
        [],
        10**6,
        (block_map, top_front.reshape(12 * 6 * G, B), arrived),
        (0,),
    )
    return (top_out.reshape(top_front.shape), solved)


def solution(mesh):
    return jax.shard_map(
        local,
        mesh=mesh,
        in_specs=(
            P("group", None, "col", None, None, "row", None),
            P(None, "col", "group", None, None, "row", None),
            P(),
            P("group"),
            P("group", None),
            P(),
        ),
        out_specs=(P(None, "col", "group", None, None, "row", None), P("group", None)),
        check_vma=False,
    )
```
